32 devices in a mesh: dp: 1 (over z), sp: 32 (over y, x, core).
Axes of the slice: x: 4, y: 4, z: 1, core: 2. Of those that a mesh axis runs over, the one named last changes fastest.
The devices are a block of a 4x4x8 slice.
Arguments:
- x_one: bfloat16 [1024, 5120], P(('dp', 'sp'))
- seg_one: int32 [1024], P(('dp', 'sp'))
- pos_one: int32 [1024], P(('dp', 'sp'))
- x_two: bfloat16 [1024, 5120], P(('dp', 'sp'))
- seg_two: int32 [1024], P(('dp', 'sp'))
- pos_two: int32 [1024], P(('dp', 'sp'))
- w_qdown: bfloat16 [5120, 1536], replicated
- gain_q: bfloat16 [1536], replicated
- w_qup: bfloat16 [1536, 24576], replicated
- w_kvdown: bfloat16 [5120, 576], replicated
- gain_kv: bfloat16 [512], replicated
- w_kvup: bfloat16 [512, 32768], replicated
- w_out: bfloat16 [16384, 5120], replicated
Outputs:
- output 1: bfloat16 [1024, 5120], P(('dp', 'sp'))
- output 2: bfloat16 [1024, 5120], P(('dp', 'sp'))
All inputs are finite; a program needn't handle non-finite values.
Results may differ from the reference program's by a relative error of at most 0.0140873.
Values are sent between devices in bfloat16 or wider.
A program may use at most 768 MiB of HBM per device.

```python
import jax
import jax.numpy as jnp
from jax import lax

TOKENS = 1024
D_MODEL = 5120
HEADS = 128
Q_LAT = 1536
KV_LAT = 512
ROPE_DIM = 64
NOPE_DIM = 128
V_DIM = 128
PROMPTS = 2
QK_DIM = NOPE_DIM + ROPE_DIM
KV_DOWN = KV_LAT + ROPE_DIM
ROPE_BASE = 10000.0
NORM_EPS = 1e-6


def draw_layout(draw_key):
    shuffled = jax.random.permutation(draw_key, TOKENS - 1) + 1
    cut_points = jnp.sort(shuffled[:PROMPTS - 1]).astype(jnp.int32)
    tok_index = jnp.arange(TOKENS, dtype=jnp.int32)
    prompt_ids = jnp.searchsorted(cut_points, tok_index, side='right').astype(jnp.int32)
    prompt_start = jnp.concatenate([jnp.zeros((1,), jnp.int32), cut_points])
    return prompt_ids, tok_index - prompt_start[prompt_ids]


def normal_weight(draw_key, arr_shape, fan_in, scale_by):
    return (jax.random.normal(draw_key, arr_shape, jnp.float32) * scale_by * fan_in ** -0.5).astype(jnp.bfloat16)


def setup_inputs(seed: int = 0, part: int = 0) -> dict:
    part_keys = jax.random.split(jax.random.fold_in(jax.random.key(seed), part), 4)
    weight_keys = jax.random.split(jax.random.key(seed + 1), 7)
    seg_one, pos_one = draw_layout(part_keys[0])
    seg_two, pos_two = draw_layout(part_keys[1])
    return {
        'x_one': jax.random.normal(part_keys[2], (TOKENS, D_MODEL), jnp.float32).astype(jnp.bfloat16),
        'seg_one': seg_one,
        'pos_one': pos_one,
        'x_two': jax.random.normal(part_keys[3], (TOKENS, D_MODEL), jnp.float32).astype(jnp.bfloat16),
        'seg_two': seg_two,
        'pos_two': pos_two,
        'w_qdown': normal_weight(weight_keys[0], (D_MODEL, Q_LAT), D_MODEL, 1.0),
        'gain_q': jax.random.uniform(weight_keys[1], (Q_LAT,), jnp.float32, 0.5, 1.5).astype(jnp.bfloat16),
        'w_qup': normal_weight(weight_keys[2], (Q_LAT, HEADS * QK_DIM), Q_LAT, 1.0),
        'w_kvdown': normal_weight(weight_keys[3], (D_MODEL, KV_DOWN), D_MODEL, 1.0),
        'gain_kv': jax.random.uniform(weight_keys[4], (KV_LAT,), jnp.float32, 0.5, 1.5).astype(jnp.bfloat16),
        'w_kvup': normal_weight(weight_keys[5], (KV_LAT, HEADS * (NOPE_DIM + V_DIM)), KV_LAT, 1.0),
        'w_out': normal_weight(weight_keys[6], (HEADS * V_DIM, D_MODEL), HEADS * V_DIM, 2.0),
    }


def rms_scale(pre_norm, gain_vec):
    mean_sq = jnp.mean(pre_norm * pre_norm, axis=-1, keepdims=True)
    return (pre_norm * lax.rsqrt(mean_sq + NORM_EPS) * gain_vec.astype(jnp.float32)).astype(jnp.bfloat16)


def rope_tables(positions):
    half_dim = ROPE_DIM // 2
    inv_freq = ROPE_BASE ** (-jnp.arange(half_dim, dtype=jnp.float32) / half_dim)
    angles = positions.astype(jnp.float32)[..., None] * inv_freq
    return jnp.cos(angles), jnp.sin(angles)


def rope_rotate(rot_in, cos_tab, sin_tab):
    half_dim = ROPE_DIM // 2
    first_half = rot_in[..., :half_dim]
    second_half = rot_in[..., half_dim:]
    return jnp.concatenate([first_half * cos_tab - second_half * sin_tab, second_half * cos_tab + first_half * sin_tab], axis=-1)


def mla_block(tokens_in, prompt_ids, positions, w_qdown, gain_q, w_qup, w_kvdown, gain_kv, w_kvup, w_out):
    q_latent = rms_scale(jnp.dot(tokens_in, w_qdown, preferred_element_type=jnp.float32), gain_q)
    kv_raw = jnp.dot(tokens_in, w_kvdown, preferred_element_type=jnp.float32)
    kv_latent = rms_scale(kv_raw[:, :KV_LAT], gain_kv)
    cos_tab, sin_tab = rope_tables(positions)
    k_rope = rope_rotate(kv_raw[:, KV_LAT:], cos_tab, sin_tab).astype(jnp.bfloat16)
    allowed = (prompt_ids[:, None] == prompt_ids[None, :]) & (positions[None, :] <= positions[:, None])
    wq_heads = w_qup.reshape(Q_LAT, HEADS, QK_DIM).transpose(1, 0, 2)
    wkv_heads = w_kvup.reshape(KV_LAT, HEADS, NOPE_DIM + V_DIM).transpose(1, 0, 2)

    def one_head(head_weights):
        wq_head, wkv_head = head_weights
        q_head = jnp.dot(q_latent, wq_head, preferred_element_type=jnp.float32)
        q_nope = q_head[:, :NOPE_DIM].astype(jnp.bfloat16)
        q_rope = rope_rotate(q_head[:, NOPE_DIM:], cos_tab, sin_tab).astype(jnp.bfloat16)
        kv_head = jnp.dot(kv_latent, wkv_head, preferred_element_type=jnp.float32).astype(jnp.bfloat16)
        q_cat = jnp.concatenate([q_nope, q_rope], axis=1)
        k_cat = jnp.concatenate([kv_head[:, :NOPE_DIM], k_rope], axis=1)
        scores = jnp.dot(q_cat, k_cat.T, preferred_element_type=jnp.float32) * QK_DIM ** -0.5
        attn_prob = jax.nn.softmax(jnp.where(allowed, scores, -1e30), axis=-1).astype(jnp.bfloat16)
        return jnp.dot(attn_prob, kv_head[:, NOPE_DIM:], preferred_element_type=jnp.float32).astype(jnp.bfloat16)

    head_out = lax.map(one_head, (wq_heads, wkv_heads))
    attn_flat = head_out.transpose(1, 0, 2).reshape(TOKENS, HEADS * V_DIM)
    return jnp.dot(attn_flat, w_out, preferred_element_type=jnp.float32).astype(jnp.bfloat16)


def reference(x_one, seg_one, pos_one, x_two, seg_two, pos_two, w_qdown, gain_q, w_qup, w_kvdown, gain_kv, w_kvup, w_out):
    y_one = mla_block(x_one, seg_one, pos_one, w_qdown, gain_q, w_qup, w_kvdown, gain_kv, w_kvup, w_out)
    y_two = mla_block(x_two, seg_two, pos_two, w_qdown, gain_q, w_qup, w_kvdown, gain_kv, w_kvup, w_out)
    return (y_one, y_two)
```

```python
import functools

import jax
import jax.numpy as jnp
from jax import lax
from jax.experimental import pallas as pl
from jax.experimental.pallas import tpu as pltpu
from jax.sharding import PartitionSpec as P

NOPE_DIM = 128
ROPE_DIM = 64
KV_LAT = 512
V_DIM = 128
QK_DIM = NOPE_DIM + ROPE_DIM
KV_HEAD = NOPE_DIM + V_DIM
ROPE_BASE = 10000.0
NORM_EPS = 1e-6
LANES = 128

CORES = 2
ROW = 4
X_BIT = CORES
Y_BIT = CORES * ROW
CHIP_MASKS = (0, X_BIT, Y_BIT, X_BIT + Y_BIT)
CHIPS = len(CHIP_MASKS)
MEMBERS = CHIPS * CORES
MICRO = 2
KV_PACK = KV_LAT + LANES
HEADS_PER_STEP = 2
CHUNKS = 2
VMEM_LIMIT = 60 * 1024 * 1024
MESH = pl.DeviceIdType.MESH


def rms_scale(pre_norm, gain_vec):
    mean_sq = jnp.mean(pre_norm * pre_norm, axis=-1, keepdims=True)
    return (pre_norm * lax.rsqrt(mean_sq + NORM_EPS) * gain_vec.astype(jnp.float32)).astype(jnp.bfloat16)


def rope_tables(positions):
    half_dim = ROPE_DIM // 2
    inv_freq = ROPE_BASE ** (-jnp.arange(half_dim, dtype=jnp.float32) / half_dim)
    angles = positions.astype(jnp.float32)[..., None] * inv_freq
    return jnp.cos(angles), jnp.sin(angles)


def rope_rotate(rot_in, cos_tab, sin_tab):
    half_dim = ROPE_DIM // 2
    first_half = rot_in[..., :half_dim]
    second_half = rot_in[..., half_dim:]
    return jnp.concatenate([first_half * cos_tab - second_half * sin_tab, second_half * cos_tab + first_half * sin_tab], axis=-1)


def gather_kernel(cq_ref, kv_ref, cq_all, kv_all, loc, cq_send, cq_recv, kv_send, kv_recv):
    me = lax.axis_index("sp")
    core = me % CORES
    chip = me // CORES
    x = chip % ROW
    y = chip // ROW
    flip_x = (1 - 2 * (x % 2))
    flip_y = (1 - 2 * (y % 2))
    sib = me + 1 - 2 * core

    def dev(dy, dx):
        return (((y + dy + ROW) % ROW) * ROW + (x + dx + ROW) % ROW) * CORES + core

    def near(first, second):
        return dev(core * first + (1 - core) * second, (1 - core) * first + core * second)

    px = dev(0, flip_x)
    py = dev(flip_y, 0)
    pd = dev(flip_y, flip_x)
    square = (me, px, py, pd)

    barrier = pltpu.get_barrier_semaphore()
    peers = [sib, pd, near(1, 0), near(-1, 0), near(0, 1), near(0, -1)]
    for peer in peers:
        pl.semaphore_signal(barrier, inc=1, device_id={"sp": peer}, device_id_type=MESH)
    pl.semaphore_wait(barrier, len(peers))

    started = []

    def send(src, dst, sems, to):
        copy = pltpu.make_async_remote_copy(
            src_ref=src, dst_ref=dst, send_sem=sems[0], recv_sem=sems[1], device_id={"sp": to}, device_id_type=MESH
        )
        copy.start()
        started.append(copy)
        return copy

    own_cq = pltpu.make_async_copy(cq_ref, cq_all.at[0, 0], loc.at[0])
    own_kv = pltpu.make_async_copy(kv_ref, kv_all.at[me], loc.at[1])
    own_cq.start()
    own_kv.start()

    cq_in = {}
    for slot in (1, 2, 3):
        cq_in[slot] = send(cq_ref, cq_all.at[slot, 0], (cq_send.at[slot], cq_recv.at[slot]), square[slot])
    send(cq_ref, cq_all.at[0, 1], (cq_send.at[CHIPS], cq_recv.at[CHIPS]), sib)

    n_kv = [0]

    def kv_sems():
        s = n_kv[0]
        n_kv[0] += 1
        return kv_send.at[s], kv_recv.at[s]

    def kv_copy(src_local, owner, to, part=None):
        if part is None:
            src = kv_ref if src_local else kv_all.at[owner]
            return send(src, kv_all.at[owner], kv_sems(), to)
        src = kv_ref.at[part] if src_local else kv_all.at[owner, part]
        return send(src, kv_all.at[owner, part], kv_sems(), to)

    right1, left1 = near(1, 0), near(-1, 0)
    right2, left2 = near(0, 1), near(0, -1)

    first_r = kv_copy(True, me, right1)
    first_l = kv_copy(True, me, left1)

    def second_start(owner, local, part=None):
        r = kv_copy(local, owner, right2, part)
        l = kv_copy(local, owner, left2, part)
        return r, l

    def second_own(f):
        return near(f, 0)

    pairs = [(0, second_start(me, True))]
    d2d = [kv_copy(True, me, sib)]
    first_r.wait_recv()
    fwd_r = kv_copy(False, near(-1, 0), right1, 0)
    pairs.append((-1, second_start(near(-1, 0), False)))
    d2d.append(kv_copy(False, near(-1, 0), sib))
    first_l.wait_recv()
    fwd_l = kv_copy(False, near(1, 0), left1, 1)
    pairs.append((1, second_start(near(1, 0), False)))
    d2d.append(kv_copy(False, near(1, 0), sib))

    for slot in (1, 2, 3):
        cq_in[slot].wait_recv()
        send(cq_all.at[slot, 0], cq_all.at[slot, 1], (cq_send.at[CHIPS + slot], cq_recv.at[CHIPS + slot]), sib)

    fwd_r.wait_recv()
    fwd_l.wait_recv()
    far = near(2, 0)
    pairs.append((2, second_start(far, False)))
    d2d.append(kv_copy(False, far, sib))

    tail = []
    for f, (r, l) in pairs:
        r.wait_recv()
        tail.append((f, kv_copy(False, near(f, -1), right2, 0), None))
        d2d.append(kv_copy(False, near(f, -1), sib))
        l.wait_recv()
        tail.append((f, kv_copy(False, near(f, 1), left2, 1), None))
        d2d.append(kv_copy(False, near(f, 1), sib))
    for i in range(0, len(tail), 2):
        f = tail[i][0]
        tail[i][1].wait_recv()
        tail[i + 1][1].wait_recv()
        d2d.append(kv_copy(False, near(f, 2), sib))

    for copy in d2d:
        copy.wait_recv()
    for copy in started:
        if copy is started[3]:
            copy.wait_recv()
    for slot in (1, 2, 3):
        pltpu.make_async_remote_copy(
            src_ref=cq_all.at[slot, 0],
            dst_ref=cq_all.at[slot, 1],
            send_sem=cq_send.at[CHIPS + slot],
            recv_sem=cq_recv.at[CHIPS + slot],
            device_id={"sp": sib},
            device_id_type=MESH,
        ).wait_recv()
    for copy in started:
        copy.wait_send()
    own_cq.wait()
    own_kv.wait()


def gather_latents(cq, kv, group):
    n_kv = 2 + 2 + 4 * 2 + 4 * 2 + group // CORES
    return pl.pallas_call(
        gather_kernel,
        out_shape=(
            jax.ShapeDtypeStruct((CHIPS, CORES) + cq.shape, cq.dtype),
            jax.ShapeDtypeStruct((group,) + kv.shape, kv.dtype),
        ),
        in_specs=[pl.BlockSpec(memory_space=pltpu.VMEM)] * 2,
        out_specs=(pl.BlockSpec(memory_space=pltpu.VMEM),) * 2,
        scratch_shapes=[
            pltpu.SemaphoreType.DMA((2,)),
            pltpu.SemaphoreType.DMA((2 * CHIPS,)),
            pltpu.SemaphoreType.DMA((2 * CHIPS,)),
            pltpu.SemaphoreType.DMA((n_kv,)),
            pltpu.SemaphoreType.DMA((n_kv,)),
        ],
        compiler_params=pltpu.CompilerParams(collective_id=0, has_side_effects=True, vmem_limit_bytes=VMEM_LIMIT),
        name="gather_latents",
    )(cq, kv)


def attention_kernel(first_pair, cq_ref, kv_ref, wq_ref, wkv_ref, cos_ref, sin_ref, qlo_ref, qhi_ref, kcode_ref, o0, o1, o2, o3, kcat_ref, v_ref, mask_ref):
    del first_pair
    outs = (o0, o1, o2, o3)
    dev, _, rows, q_lat = cq_ref.shape[1:] if False else (kv_ref.shape[0], None, kv_ref.shape[2], cq_ref.shape[-1])
    keys = dev * rows
    q_rows = MEMBERS * rows

    @pl.when(pl.program_id(0) == 0)
    def _():
        for mb in range(MICRO):
            kcat_ref[mb, :, NOPE_DIM:] = kv_ref[:, mb, :, KV_LAT:].reshape(keys, LANES)
            code = kcode_ref[mb]
            keep = (code >= qlo_ref[mb]) & (code <= qhi_ref[mb])
            mask_ref[mb] = jnp.where(keep, 1.0, 0.0)

    cq = cq_ref[...].reshape(MEMBERS * MICRO * rows, q_lat)
    latent = kv_ref[...].reshape(dev * MICRO * rows, KV_PACK)[:, :KV_LAT]
    for hh in range(HEADS_PER_STEP):
        kv = jnp.dot(latent, wkv_ref[:, hh * KV_HEAD:(hh + 1) * KV_HEAD], preferred_element_type=jnp.float32)
        kv = kv.astype(jnp.bfloat16).reshape(dev, MICRO, rows, KV_HEAD)
        for mb in range(MICRO):
            one = kv[:, mb].reshape(keys, KV_HEAD)
            kcat_ref[mb, :, :NOPE_DIM] = one[:, :NOPE_DIM]
            v_ref[mb] = one[:, NOPE_DIM:]
        f = jnp.dot(cq, wq_ref[:, hh * QK_DIM:(hh + 1) * QK_DIM], preferred_element_type=jnp.float32)
        z = f[:, NOPE_DIM:]
        turned = jnp.concatenate([z[:, ROPE_DIM // 2:], z[:, :ROPE_DIM // 2]], axis=1)
        rot = z * cos_ref[...] + turned * sin_ref[...]
        pad = jnp.zeros((rot.shape[0], LANES - ROPE_DIM), jnp.float32)
        q = jnp.concatenate([f[:, :NOPE_DIM], rot, pad], axis=1).astype(jnp.bfloat16)
        q = q.reshape(MEMBERS, MICRO, rows, NOPE_DIM + LANES)
        for mb in range(MICRO):
            s = lax.dot_general(
                q[:, mb].reshape(q_rows, NOPE_DIM + LANES), kcat_ref[mb], (((1,), (1,)), ((), ())), preferred_element_type=jnp.float32
            )
            s = jnp.where(mask_ref[mb] > 0.5, s * QK_DIM ** -0.5, -1e30)
            e = jnp.exp(s - jnp.max(s, axis=1, keepdims=True))
            p = (e * (1.0 / jnp.sum(e, axis=1, keepdims=True))).astype(jnp.bfloat16)
            o = jnp.dot(p, v_ref[mb], preferred_element_type=jnp.float32).astype(jnp.bfloat16)
            o = o.reshape(CHIPS, CORES, rows, V_DIM)
            for d in range(CHIPS):
                outs[d][:, mb, :, hh * V_DIM:(hh + 1) * V_DIM] = o[d]


def attention(first_pair, cq_all, kv_all, w_qup, w_kvup, cos_q, sin_q, q_lo, q_hi, k_code, steps):
    rows = kv_all.shape[2]
    keys = kv_all.shape[0] * rows
    hw = HEADS_PER_STEP
    full = lambda a: pl.BlockSpec(a.shape, lambda i, s, n=a.ndim: (0,) * n)
    out = jax.ShapeDtypeStruct((CORES, MICRO, rows, steps * hw * V_DIM), jnp.bfloat16)
    flops = 2 * steps * hw * (MEMBERS * MICRO * rows * cq_all.shape[-1] * QK_DIM + MICRO * keys * KV_LAT * KV_HEAD + 2 * MICRO * MEMBERS * rows * keys * 256)
    return pl.pallas_call(
        attention_kernel,
        grid_spec=pltpu.PrefetchScalarGridSpec(
            num_scalar_prefetch=1,
            grid=(steps,),
            in_specs=[
                full(cq_all),
                full(kv_all),
                pl.BlockSpec((w_qup.shape[0], hw * QK_DIM), lambda i, s: (0, s[0] + i)),
                pl.BlockSpec((w_kvup.shape[0], hw * KV_HEAD), lambda i, s: (0, s[0] + i)),
                full(cos_q),
                full(sin_q),
                full(q_lo),
                full(q_hi),
                full(k_code),
            ],
            out_specs=[pl.BlockSpec((CORES, MICRO, rows, hw * V_DIM), lambda i, s: (0, 0, 0, i))] * CHIPS,
            scratch_shapes=[
                pltpu.VMEM((MICRO, keys, NOPE_DIM + LANES), jnp.bfloat16),
                pltpu.VMEM((MICRO, keys, V_DIM), jnp.bfloat16),
                pltpu.VMEM((MICRO, MEMBERS * rows, keys), jnp.float32),
            ],
        ),
        out_shape=[out] * CHIPS,
        compiler_params=pltpu.CompilerParams(dimension_semantics=("arbitrary",), vmem_limit_bytes=VMEM_LIMIT),
        cost_estimate=pl.CostEstimate(flops=flops, bytes_accessed=steps * hw * 2 * (1536 * 192 + 512 * 256), transcendentals=0),
        name="attention",
    )(first_pair, cq_all, kv_all, w_qup, w_kvup, cos_q, sin_q, q_lo, q_hi, k_code)


def out_kernel(k_blocks, per_piece, *refs):
    piece_refs = refs[:CHIPS]
    w_ref = refs[CHIPS]
    acc_in = refs[CHIPS + 1:-1] if len(refs) > CHIPS + 2 else ()
    y_ref = refs[-1]
    i = pl.program_id(0)
    rows = y_ref.shape[0]
    blk = w_ref.shape[0]

    def product(d):
        return jnp.dot(piece_refs[d][...].reshape(rows, blk), w_ref[...], preferred_element_type=jnp.float32)

    for d in range(CHIPS):
        @pl.when(i // per_piece == d)
        def _(d=d):
            if d == 0:
                @pl.when(i == 0)
                def _():
                    base = product(0)
                    y_ref[...] = base + acc_in[0][...] if acc_in else base
                @pl.when(i > 0)
                def _():
                    y_ref[...] += product(0)
            else:
                y_ref[...] += product(d)


def out_project(w_rows, pieces, w_out, acc):
    rows = CORES * MICRO * pieces[0].shape[2]
    depth = pieces[0].shape[3]
    blk = 512
    per_piece = depth // blk
    steps = CHIPS * per_piece
    cols = w_out.shape[1]

    def kern(s, *refs):
        return out_kernel(steps, per_piece, *refs)

    piece_specs = [
        pl.BlockSpec(pieces[0].shape[:3] + (blk,), lambda i, s, d=d: (0, 0, 0, jnp.clip(i - d * per_piece, 0, per_piece - 1)))
        for d in range(CHIPS)
    ]
    extra = [] if acc is None else [acc]
    return pl.pallas_call(
        kern,
        grid_spec=pltpu.PrefetchScalarGridSpec(
            num_scalar_prefetch=1,
            grid=(steps,),
            in_specs=piece_specs
            + [pl.BlockSpec((blk, cols), lambda i, s: (s[i // per_piece] + i % per_piece, 0))]
            + [pl.BlockSpec((rows, cols), lambda i, s: (0, 0))] * len(extra),
            out_specs=pl.BlockSpec((rows, cols), lambda i, s: (0, 0)),
        ),
        out_shape=jax.ShapeDtypeStruct((rows, cols), jnp.float32),
        compiler_params=pltpu.CompilerParams(dimension_semantics=("arbitrary",), vmem_limit_bytes=VMEM_LIMIT),
        cost_estimate=pl.CostEstimate(flops=2 * rows * CHIPS * depth * cols, bytes_accessed=2 * CHIPS * depth * cols, transcendentals=0),
        name="out_project",
    )(w_rows, *pieces, w_out, *extra)


def solution(mesh):
    tok_spec = P(("dp", "sp"), None)
    idx_spec = P(("dp", "sp"))
    group = mesh.shape["sp"]

    def flip_perm(mask):
        return [(i, i ^ mask) for i in range(group)]

    def local_body(x_one, seg_one, pos_one, x_two, seg_two, pos_two, w_qdown, gain_q, w_qup, w_kvdown, gain_kv, w_kvup, w_out):
        rows = x_one.shape[0]
        heads = w_out.shape[0] // V_DIM
        my_heads = heads // MEMBERS
        me = lax.axis_index("sp")
        core = me % CORES
        chip_in_square = (me // X_BIT) % 2 + 2 * ((me // Y_BIT) % 2)

        x_both = jnp.concatenate([x_one, x_two], axis=0)
        pos = jnp.concatenate([pos_one, pos_two])
        seg = jnp.concatenate([seg_one, seg_two])
        kv_raw = jnp.dot(x_both, w_kvdown, preferred_element_type=jnp.float32)
        kv_latent = rms_scale(kv_raw[:, :KV_LAT], gain_kv)
        cos_k, sin_k = rope_tables(pos)
        k_rope = rope_rotate(kv_raw[:, KV_LAT:], cos_k, sin_k).astype(jnp.bfloat16)
        q_latent = rms_scale(jnp.dot(x_both, w_qdown, preferred_element_type=jnp.float32), gain_q)
        meta = jnp.stack([seg, pos // 32, pos % 32], axis=1).astype(jnp.bfloat16)
        meta = jnp.pad(meta, ((0, 0), (0, LANES - ROPE_DIM - 3)))
        packed = jnp.concatenate([kv_latent, k_rope, meta], axis=1).reshape(MICRO, rows, KV_PACK)
        cq_all, kv_all = gather_latents(q_latent.reshape(MICRO, rows, -1), packed, group)

        tags = kv_all[..., KV_LAT + ROPE_DIM:KV_LAT + ROPE_DIM + 3].astype(jnp.int32)
        seg_all = tags[..., 0]
        pos_all = tags[..., 1] * 32 + tags[..., 2]
        limit = group * rows
        code = seg_all * limit + pos_all
        k_code = code.transpose(1, 0, 2).reshape(MICRO, 1, group * rows)
        members = jnp.stack([jnp.bitwise_xor(me, mask + c) for mask in CHIP_MASKS for c in range(CORES)])
        q_pos = pos_all[members]
        q_hi = code[members].transpose(1, 0, 2).reshape(MICRO, MEMBERS * rows, 1)
        q_lo = q_hi - q_pos.transpose(1, 0, 2).reshape(MICRO, MEMBERS * rows, 1)
        cos_q, sin_q = rope_tables(q_pos.reshape(-1))
        cos_q = jnp.concatenate([cos_q, cos_q], axis=1)
        sin_q = jnp.concatenate([-sin_q, sin_q], axis=1)

        head0 = core * (heads // CORES) + chip_in_square * my_heads
        chunk_heads = my_heads // CHUNKS
        steps = chunk_heads // HEADS_PER_STEP
        blk = 512
        acc = None
        all_pieces = []
        for j in range(CHUNKS):
            first_pair = ((head0 + j * chunk_heads) // HEADS_PER_STEP).astype(jnp.int32).reshape(1)
            outs = attention(first_pair, cq_all, kv_all, w_qup, w_kvup, cos_q, sin_q, q_lo, q_hi, k_code, steps)
            pieces = [outs[0]] + [lax.ppermute(outs[d], "sp", flip_perm(CHIP_MASKS[d])) for d in range(1, CHIPS)]
            all_pieces.append(pieces)
        for j in range(CHUNKS):
            owners = [core * (heads // CORES) + jnp.bitwise_xor(chip_in_square, d) * my_heads + j * chunk_heads for d in range(CHIPS)]
            w_rows = (jnp.stack(owners) * V_DIM // blk).astype(jnp.int32)
            acc = out_project(w_rows, all_pieces[j], w_out, acc)
        y_rows = MICRO * rows
        other = lax.ppermute(acc[y_rows:], "sp", flip_perm(1))
        y = (acc[:y_rows] + other).astype(jnp.bfloat16)
        return y[:rows], y[rows:]

    rep = P()
    return jax.shard_map(
        local_body,
        mesh=mesh,
        in_specs=(tok_spec, idx_spec, idx_spec, tok_spec, idx_spec, idx_spec, rep, rep, rep, rep, rep, rep, rep),
        out_specs=(tok_spec, tok_spec),
        check_vma=False,
    )
```

```python
import functools

import jax
import jax.numpy as jnp
from jax import lax
from jax.experimental import pallas as pl
from jax.experimental.pallas import tpu as pltpu
from jax.sharding import PartitionSpec as P

NOPE_DIM = 128
ROPE_DIM = 64
KV_LAT = 512
V_DIM = 128
QK_DIM = NOPE_DIM + ROPE_DIM
KV_HEAD = NOPE_DIM + V_DIM
ROPE_BASE = 10000.0
NORM_EPS = 1e-6
LANES = 128

CORES = 2
ROW = 4
CHIPS = 4
MEMBERS = CHIPS * CORES
MICRO = 2
KV_PACK = KV_LAT + LANES
HEADS_PER_STEP = 2
SOFT_ROWS = 16
OUT_COLS = 256
OUT_SLOTS = 7
LAG = 3
VMEM_LIMIT = 67_043_328
MESH = pl.DeviceIdType.MESH


def rms_scale(pre_norm, gain_vec):
    mean_sq = jnp.mean(pre_norm * pre_norm, axis=-1, keepdims=True)
    return (pre_norm * lax.rsqrt(mean_sq + NORM_EPS) * gain_vec.astype(jnp.float32)).astype(jnp.bfloat16)


def rope_tables(positions):
    half_dim = ROPE_DIM // 2
    inv_freq = ROPE_BASE ** (-jnp.arange(half_dim, dtype=jnp.float32) / half_dim)
    angles = positions.astype(jnp.float32)[..., None] * inv_freq
    return jnp.cos(angles), jnp.sin(angles)


def rope_rotate(rot_in, cos_tab, sin_tab):
    half_dim = ROPE_DIM // 2
    first_half = rot_in[..., :half_dim]
    second_half = rot_in[..., half_dim:]
    return jnp.concatenate([first_half * cos_tab - second_half * sin_tab, second_half * cos_tab + first_half * sin_tab], axis=-1)


def place():
    me = lax.axis_index("sp")
    core = me % CORES
    chip = me // CORES
    x = chip % ROW
    y = chip // ROW

    def dev(dy, dx):
        return (((y + dy + ROW) % ROW) * ROW + (x + dx + ROW) % ROW) * CORES + core

    def near(first, second):
        return dev(core * first + (1 - core) * second, (1 - core) * first + core * second)

    flip_x = 1 - 2 * (x % 2)
    flip_y = 1 - 2 * (y % 2)
    square = (me, dev(0, flip_x), dev(flip_y, 0), dev(flip_y, flip_x))
    corner = tuple((d % 2) * (1 - x % 2) + (1 - d % 2) * (x % 2) + 2 * ((d // 2) * (1 - y % 2) + (1 - d // 2) * (y % 2)) for d in range(CHIPS))
    return me, core, me + 1 - 2 * core, square, corner, near


def meet(peers):
    barrier = pltpu.get_barrier_semaphore()
    for peer in peers:
        pl.semaphore_signal(barrier, inc=1, device_id={"sp": peer}, device_id_type=MESH)
    pl.semaphore_wait(barrier, len(peers))


def gather(where, cq_ref, kv_ref, tab_ref, cq_all, kv_all, tab_all, loc, send_sems, recv_sems):
    me, _, sib, square, _, near = where
    right1, left1, right2, left2 = near(1, 0), near(-1, 0), near(0, 1), near(0, -1)
    copies = []

    def send(src, dst, to):
        n = len(copies)
        copy = pltpu.make_async_remote_copy(
            src_ref=src, dst_ref=dst, send_sem=send_sems.at[n], recv_sem=recv_sems.at[n], device_id={"sp": to}, device_id_type=MESH
        )
        copy.start()
        copies.append(copy)
        return copy

    handed = []

    def send_kv(owner, to, part=None):
        at = (owner,) if part is None else (owner, part)
        return send(kv_all.at[at], kv_all.at[at], to)

    def hand_kv(owner):
        handed.append(send_kv(owner, sib))

    def hand(slot):
        handed.append(send(cq_all.at[slot, 0], cq_all.at[slot, 1], sib))
        handed.append(send(tab_all.at[slot, 0], tab_all.at[slot, 1], sib))

    own = (
        pltpu.make_async_copy(kv_ref, kv_all.at[me], loc.at[0]),
        pltpu.make_async_copy(cq_ref, cq_all.at[0, 0], loc.at[1]),
        pltpu.make_async_copy(tab_ref, tab_all.at[0, 0], loc.at[2]),
    )
    for copy in own:
        copy.start()
    first_r = send(kv_ref, kv_all.at[me], right1)
    first_l = send(kv_ref, kv_all.at[me], left1)
    second = {0: (send(kv_ref, kv_all.at[me], right2), send(kv_ref, kv_all.at[me], left2))}
    tab_in = {s: send(tab_ref, tab_all.at[s, 0], square[s]) for s in (1, 2, 3)}
    cq_in = {s: send(cq_ref, cq_all.at[s, 0], square[s]) for s in (1, 2)}
    handed.append(send(kv_ref, kv_all.at[me], sib))
    handed.append(send(cq_ref, cq_all.at[0, 1], sib))
    handed.append(send(tab_ref, tab_all.at[0, 1], sib))

    first_r.wait_recv()
    far_r = send_kv(left1, right1, 0)
    second[-1] = (send_kv(left1, right2), send_kv(left1, left2))
    hand_kv(left1)
    first_l.wait_recv()
    far_l = send_kv(right1, left1, 1)
    second[1] = (send_kv(right1, right2), send_kv(right1, left2))
    hand_kv(right1)

    def pass_on(first):
        r, l = second[first]
        below, above = near(first, -1), near(first, 1)
        r.wait_recv()
        up = send_kv(below, right2, 0)
        hand_kv(below)
        l.wait_recv()
        down = send_kv(above, left2, 1)
        hand_kv(above)
        return up, down

    last = {0: pass_on(0)}
    far = near(2, 0)
    far_r.wait_recv()
    far_l.wait_recv()
    second[2] = (send_kv(far, right2), send_kv(far, left2))
    hand_kv(far)

    cq_in[1].wait_recv()
    tab_in[1].wait_recv()
    diag_a = send(cq_all.at[1, 0, 0], cq_all.at[3, 0, 0], square[2])
    hand(1)
    cq_in[2].wait_recv()
    tab_in[2].wait_recv()
    diag_b = send(cq_all.at[2, 0, 1], cq_all.at[3, 0, 1], square[1])
    hand(2)

    for first in (-1, 1, 2):
        last[first] = pass_on(first)
    diag_a.wait_recv()
    diag_b.wait_recv()
    tab_in[3].wait_recv()
    hand(3)
    for first in (0, -1, 1, 2):
        for copy in last[first]:
            copy.wait_recv()
        hand_kv(near(first, 2))
    for copy in handed:
        copy.wait_recv()
    for copy in copies:
        copy.wait_send()
    for copy in own:
        copy.wait()


N_COPIES = 4 + 3 + 2 + 3 + 2 + 4 * 2 + 2 * 3 + 15 + 2 + 6


def block_kernel(
    cq_ref, kv_ref0, tab_ref0, wqup_ref, wkvup_ref, wout_ref, y1_ref, y2_ref,
    cq_ref_all, kv_ref, tab_ref, wq_buf, wkv_buf, wo_buf, o_ref, o_in, y_own, y_far, y_in,
    kcat_ref, v_ref, qcat_ref, s_ref, p_ref, mask_ref,
    loc, g_send, g_recv, w_sem, wo_sem, o_send_sem, o_recv_sem, y_send_sem, y_recv_sem,
):
    where = place()
    me, core, sib, square, corner, near = where
    devs, _, rows, _ = kv_ref.shape
    keys = devs * rows
    q_lat = cq_ref_all.shape[-1]
    chip_rows = CORES * rows
    q_rows = CHIPS * chip_rows
    key_devs = devs // 8
    key_chunk = key_devs * rows
    soft_rows = SOFT_ROWS
    steps = o_ref.shape[1]
    heads = wqup_ref.shape[1] // QK_DIM
    my_heads = heads // MEMBERS
    n_blocks, _, blk = y_in.shape
    slots = wo_buf.shape[0]
    to_exp2 = QK_DIM ** -0.5 * 1.4426950408889634

    def first_head(d):
        return core * (heads // CORES) + corner[d] * my_heads

    def weight_copies(i):
        slot = i % 2
        h = first_head(0) + HEADS_PER_STEP * i
        wq, wkv = HEADS_PER_STEP * QK_DIM, HEADS_PER_STEP * KV_HEAD
        return (
            pltpu.make_async_copy(wqup_ref.at[:, pl.ds(pl.multiple_of(h * QK_DIM, LANES), wq)], wq_buf.at[slot], w_sem.at[slot, 0]),
            pltpu.make_async_copy(wkvup_ref.at[:, pl.ds(pl.multiple_of(h * KV_HEAD, LANES), wkv)], wkv_buf.at[slot], w_sem.at[slot, 1]),
        )

    def out_copies(b):
        slot = b % slots
        depth = my_heads * V_DIM
        return [
            pltpu.make_async_copy(
                wout_ref.at[pl.ds(pl.multiple_of(first_head(d) * V_DIM, depth), depth), pl.ds(pl.multiple_of(b * blk, LANES), blk)],
                wo_buf.at[slot, d],
                wo_sem.at[slot, d],
            )
            for d in range(CHIPS)
        ]

    for copy in weight_copies(0):
        copy.start()

    @pl.loop(0, slots)
    def _(b):
        for copy in out_copies(b):
            copy.start()

    meet((sib, square[3], near(1, 0), near(-1, 0), near(0, 1), near(0, -1)))
    gather(where, cq_ref, kv_ref0, tab_ref0, cq_ref_all, kv_ref, tab_ref, loc, g_send, g_recv)

    lane = lax.broadcasted_iota(jnp.int32, (LANES, LANES), 1)
    weight = jnp.where(lane == ROPE_DIM, float(keys), jnp.where(lane == ROPE_DIM + 1, 32.0, jnp.where(lane == ROPE_DIM + 2, 1.0, 0.0)))
    weight_pos = jnp.where(lane == ROPE_DIM, 0.0, weight)
    nt = (((1,), (1,)), ((), ()))
    for mb in range(MICRO):
        tail = kv_ref[:, mb, :, KV_LAT:].reshape(keys, LANES)
        for par in range(HEADS_PER_STEP):
            kcat_ref[par, mb, :, NOPE_DIM:] = tail
        k_code = lax.dot_general(weight.astype(jnp.bfloat16), tail, nt, preferred_element_type=jnp.float32)
        for r in range(MEMBERS):
            owner = square[r // CORES] + (r % CORES) * (1 - 2 * core)
            mine = kv_ref[owner, mb, :, KV_LAT:]
            q_code = lax.dot_general(mine, weight.astype(jnp.bfloat16), nt, preferred_element_type=jnp.float32)
            q_pos = lax.dot_general(mine, weight_pos.astype(jnp.bfloat16), nt, preferred_element_type=jnp.float32)
            hi = q_code[:, :1]
            lo = (q_code - q_pos)[:, :1]
            row = k_code[:1, :]
            mask_ref[mb, r * rows:(r + 1) * rows, :] = jnp.where((row >= lo) & (row <= hi), 1.0, 0.0)

    def kv_part(slot, par, c):
        latent = kv_ref[c * key_devs:(c + 1) * key_devs, :, :, :KV_LAT].reshape(key_devs * MICRO * rows, KV_LAT)
        kv = jnp.dot(latent, wkv_buf[slot, :, par * KV_HEAD:(par + 1) * KV_HEAD], preferred_element_type=jnp.float32)
        kv = kv.astype(jnp.bfloat16).reshape(key_devs, MICRO, rows, KV_HEAD)
        for mb in range(MICRO):
            one = kv[:, mb].reshape(key_chunk, KV_HEAD)
            kcat_ref[par, mb, c * key_chunk:(c + 1) * key_chunk, :NOPE_DIM] = one[:, :NOPE_DIM]
            v_ref[par, mb, c * key_chunk:(c + 1) * key_chunk, :] = one[:, NOPE_DIM:]

    def q_part(slot, par, d):
        cq = cq_ref_all[d].reshape(CORES * MICRO * rows, q_lat)
        f = jnp.dot(cq, wq_buf[slot, :, par * QK_DIM:(par + 1) * QK_DIM], preferred_element_type=jnp.float32)
        tab = tab_ref[d].reshape(CORES * MICRO * rows, 2 * ROPE_DIM)
        z = f[:, NOPE_DIM:]
        turned = jnp.concatenate([z[:, ROPE_DIM // 2:], z[:, :ROPE_DIM // 2]], axis=1)
        rot = z * tab[:, :ROPE_DIM] + turned * tab[:, ROPE_DIM:]
        pad = jnp.zeros((rot.shape[0], LANES - ROPE_DIM), jnp.float32)
        q = jnp.concatenate([f[:, :NOPE_DIM], rot, pad], axis=1).astype(jnp.bfloat16)
        q = q.reshape(CORES, MICRO, rows, NOPE_DIM + LANES)
        for mb in range(MICRO):
            qcat_ref[par, mb, d * chip_rows:(d + 1) * chip_rows, :] = q[:, mb].reshape(chip_rows, NOPE_DIM + LANES)

    def score_part(par, mb, n):
        cols = slice(n * 256, (n + 1) * 256)
        s_ref[par, mb, :, cols] = lax.dot_general(
            qcat_ref[par, mb], kcat_ref[par, mb, cols, :], (((1,), (1,)), ((), ())), preferred_element_type=jnp.float32
        )

    def soft_part(par, mb, r):
        at = slice(r * soft_rows, (r + 1) * soft_rows)
        s = jnp.where(mask_ref[mb, at, :] > 0.5, s_ref[par, mb, at, :], -1e30)
        e = jnp.exp2((s - jnp.max(s, axis=1, keepdims=True)) * to_exp2)
        p_ref[mb, at, :] = (e * (1.0 / jnp.sum(e, axis=1, keepdims=True))).astype(jnp.bfloat16)

    def value_part(par, mb, step):
        o = jnp.dot(p_ref[mb], v_ref[par, mb], preferred_element_type=jnp.float32).astype(jnp.bfloat16)
        o = o.reshape(CHIPS, CORES, rows, V_DIM)
        for d in range(CHIPS):
            o_ref[d, step, :, mb, :, par * V_DIM:(par + 1) * V_DIM] = o[d]

    def first_stage(slot, par):
        parts = [functools.partial(kv_part, slot, par, c) for c in range(8)]
        parts += [functools.partial(q_part, slot, par, d) for d in range(CHIPS)]
        parts += [functools.partial(score_part, par, mb, n) for mb in range(MICRO) for n in range(keys // 256)]
        return parts

    def second_stage(par, step):
        parts = []
        for mb in range(MICRO):
            parts += [functools.partial(soft_part, par, mb, r) for r in range(q_rows // soft_rows)]
            parts.append(functools.partial(value_part, par, mb, step))
        return parts

    def o_copies(step):
        return [
            pltpu.make_async_remote_copy(
                src_ref=o_ref.at[d, step],
                dst_ref=o_in.at[d - 1, step],
                send_sem=o_send_sem.at[d - 1, step],
                recv_sem=o_recv_sem.at[d - 1, step],
                device_id={"sp": square[d]},
                device_id_type=MESH,
            )
            for d in range(1, CHIPS)
        ]

    def beside(a, b):
        order = [((k + 0.5) / len(a), 0, f) for k, f in enumerate(a)] + [((k + 0.6) / len(b), 1, f) for k, f in enumerate(b)]
        for _, _, f in sorted(order, key=lambda v: v[:2]):
            f()

    @pl.loop(0, steps)
    def _(i):
        slot = i % 2
        before = jnp.maximum(i - 1, 0)
        for copy in weight_copies(i):
            copy.wait()

        @pl.when(i + 1 < steps)
        def _():
            for copy in weight_copies(i + 1):
                copy.start()

        beside(first_stage(slot, 0), second_stage(1, before))

        @pl.when(i > 0)
        def _():
            for copy in o_copies(before):
                copy.start()

        beside(first_stage(slot, 1), second_stage(0, i))

    for f in second_stage(1, steps - 1):
        f()
    for copy in o_copies(steps - 1):
        copy.start()

    @pl.loop(0, steps)
    def _(i):
        for copy in o_copies(i):
            copy.wait()

    def y_copy(b):
        return pltpu.make_async_remote_copy(
            src_ref=y_far.at[b], dst_ref=y_in.at[b], send_sem=y_send_sem.at[b], recv_sem=y_recv_sem.at[b], device_id={"sp": sib}, device_id_type=MESH
        )

    def finish(b):
        y_copy(b).wait()
        y = (y_own[b] + y_in[b]).astype(jnp.bfloat16)
        at = pl.ds(pl.multiple_of(b * blk, LANES), blk)
        y1_ref[:, at] = y[:rows]
        y2_ref[:, at] = y[rows:]

    @pl.loop(0, n_blocks)
    def _(b):
        slot = b % slots
        for copy in out_copies(b):
            copy.wait()
        total = None
        for d in range(CHIPS):
            src = o_ref.at[0] if d == 0 else o_in.at[d - 1]
            o = jnp.concatenate([src[s].reshape(CORES * MICRO * rows, HEADS_PER_STEP * V_DIM) for s in range(steps)], axis=1)
            term = jnp.dot(o, wo_buf[slot, d], preferred_element_type=jnp.float32)
            total = term if total is None else total + term
        y_own[b] = total[:MICRO * rows]
        y_far[b] = total[MICRO * rows:]
        y_copy(b).start()

        @pl.when(b + slots < n_blocks)
        def _():
            for copy in out_copies(b + slots):
                copy.start()

        @pl.when(b >= LAG)
        def _():
            finish(b - LAG)

    @pl.loop(n_blocks - LAG, n_blocks)
    def _(b):
        finish(b)


def latent_block(cq, kv, table, w_qup, w_kvup, w_out, group):
    rows = kv.shape[1]
    keys = group * rows
    q_rows = MEMBERS * rows
    hw = HEADS_PER_STEP
    heads = w_out.shape[0] // V_DIM
    steps = heads // MEMBERS // hw
    cols = w_out.shape[1]
    n_blocks = cols // OUT_COLS
    out = jax.ShapeDtypeStruct((rows, cols), jnp.bfloat16)
    dma = pltpu.SemaphoreType.DMA
    vmem, anywhere = pl.BlockSpec(memory_space=pltpu.VMEM), pl.BlockSpec(memory_space=pl.ANY)
    pair = (steps, CORES, MICRO, rows, hw * V_DIM)
    bf16, f32 = jnp.bfloat16, jnp.float32
    return pl.pallas_call(
        block_kernel,
        out_shape=(out, out),
        in_specs=[vmem] * 3 + [anywhere] * 3,
        out_specs=(vmem, vmem),
        scratch_shapes=[
            pltpu.VMEM((CHIPS, CORES) + cq.shape, bf16),
            pltpu.VMEM((group,) + kv.shape, bf16),
            pltpu.VMEM((CHIPS, CORES) + table.shape, f32),
            pltpu.VMEM((2, w_qup.shape[0], hw * QK_DIM), bf16),
            pltpu.VMEM((2, w_kvup.shape[0], hw * KV_HEAD), bf16),
            pltpu.VMEM((OUT_SLOTS, CHIPS, heads // MEMBERS * V_DIM, OUT_COLS), bf16),
            pltpu.VMEM((CHIPS,) + pair, bf16),
            pltpu.VMEM((CHIPS - 1,) + pair, bf16),
            pltpu.VMEM((n_blocks, MICRO * rows, OUT_COLS), f32),
            pltpu.VMEM((n_blocks, MICRO * rows, OUT_COLS), f32),
            pltpu.VMEM((n_blocks, MICRO * rows, OUT_COLS), f32),
            pltpu.VMEM((hw, MICRO, keys, NOPE_DIM + LANES), bf16),
            pltpu.VMEM((hw, MICRO, keys, V_DIM), bf16),
            pltpu.VMEM((hw, MICRO, q_rows, NOPE_DIM + LANES), bf16),
            pltpu.VMEM((hw, MICRO, q_rows, keys), f32),
            pltpu.VMEM((MICRO, q_rows, keys), bf16),
            pltpu.VMEM((MICRO, q_rows, keys), f32),
            dma((3,)),
            dma((N_COPIES,)),
            dma((N_COPIES,)),
            dma((2, 2)),
            dma((OUT_SLOTS, CHIPS)),
            dma((CHIPS - 1, steps)),
            dma((CHIPS - 1, steps)),
            dma((n_blocks,)),
            dma((n_blocks,)),
        ],
        compiler_params=pltpu.CompilerParams(collective_id=0, has_side_effects=True, vmem_limit_bytes=VMEM_LIMIT),
        name="latent_block",
    )(cq, kv, table, w_qup, w_kvup, w_out)


def solution(mesh):
    tok_spec = P(("dp", "sp"), None)
    idx_spec = P(("dp", "sp"))
    group = mesh.shape["sp"]

    def local_body(x_one, seg_one, pos_one, x_two, seg_two, pos_two, w_qdown, gain_q, w_qup, w_kvdown, gain_kv, w_kvup, w_out):
        rows = x_one.shape[0]
        x_both = jnp.concatenate([x_one, x_two], axis=0)
        pos = jnp.concatenate([pos_one, pos_two])
        seg = jnp.concatenate([seg_one, seg_two])
        kv_raw = jnp.dot(x_both, w_kvdown, preferred_element_type=jnp.float32)
        kv_latent = rms_scale(kv_raw[:, :KV_LAT], gain_kv)
        cos_k, sin_k = rope_tables(pos)
        k_rope = rope_rotate(kv_raw[:, KV_LAT:], cos_k, sin_k).astype(jnp.bfloat16)
        q_latent = rms_scale(jnp.dot(x_both, w_qdown, preferred_element_type=jnp.float32), gain_q)
        meta = jnp.stack([seg, pos // 32, pos % 32], axis=1).astype(jnp.bfloat16)
        meta = jnp.pad(meta, ((0, 0), (0, LANES - ROPE_DIM - 3)))
        packed = jnp.concatenate([kv_latent, k_rope, meta], axis=1).reshape(MICRO, rows, KV_PACK)
        table = jnp.concatenate([cos_k, cos_k, -sin_k, sin_k], axis=1).reshape(MICRO, rows, 2 * ROPE_DIM)
        return latent_block(q_latent.reshape(MICRO, rows, -1), packed, table, w_qup, w_kvup, w_out, group)

    rep = P()
    return jax.shard_map(
        local_body,
        mesh=mesh,
        in_specs=(tok_spec, idx_spec, idx_spec, tok_spec, idx_spec, idx_spec, rep, rep, rep, rep, rep, rep, rep),
        out_specs=(tok_spec, tok_spec),
        check_vma=False,
    )
```

```python
import functools

import jax
import jax.numpy as jnp
import numpy as np
from jax import lax
from jax.experimental import pallas as pl
from jax.experimental.pallas import tpu as pltpu
from jax.sharding import PartitionSpec as P

NOPE_DIM = 128
ROPE_DIM = 64
KV_LAT = 512
V_DIM = 128
QK_DIM = NOPE_DIM + ROPE_DIM
KV_HEAD = NOPE_DIM + V_DIM
ROPE_BASE = 10000.0
NORM_EPS = 1e-6
LANES = 128

CORES = 2
ROW = 4
CHIPS = 4
MEMBERS = CHIPS * CORES
MICRO = 2
KV_PACK = KV_LAT + LANES
HEADS_PER_STEP = 2
SOFT_ROWS = 16
OUT_COLS = 256
OUT_SLOTS = 6
LAG = 3
VMEM_LIMIT = 67_043_328
MESH = pl.DeviceIdType.MESH


def place():
    me = lax.axis_index("sp")
    core = me % CORES
    chip = me // CORES
    x = chip % ROW
    y = chip // ROW

    def dev(dy, dx):
        return (((y + dy + ROW) % ROW) * ROW + (x + dx + ROW) % ROW) * CORES + core

    def near(first, second):
        return dev(core * first + (1 - core) * second, (1 - core) * first + core * second)

    flip_x = 1 - 2 * (x % 2)
    flip_y = 1 - 2 * (y % 2)
    square = (me, dev(0, flip_x), dev(flip_y, 0), dev(flip_y, flip_x))
    corner = tuple((d % 2) * (1 - x % 2) + (1 - d % 2) * (x % 2) + 2 * ((d // 2) * (1 - y % 2) + (1 - d // 2) * (y % 2)) for d in range(CHIPS))
    return me, core, me + 1 - 2 * core, square, corner, near


def meet(peers):
    barrier = pltpu.get_barrier_semaphore()
    for peer in peers:
        pl.semaphore_signal(barrier, inc=1, device_id={"sp": peer}, device_id_type=MESH)
    pl.semaphore_wait(barrier, len(peers))


def gather(where, cq_ref, kv_ref, tab_ref, cq_all, kv_all, tab_all, loc, send_sems, recv_sems):
    me, _, sib, square, _, near = where
    right1, left1, right2, left2 = near(1, 0), near(-1, 0), near(0, 1), near(0, -1)
    copies = []

    def send(src, dst, to):
        n = len(copies)
        copy = pltpu.make_async_remote_copy(
            src_ref=src, dst_ref=dst, send_sem=send_sems.at[n], recv_sem=recv_sems.at[n], device_id={"sp": to}, device_id_type=MESH
        )
        copy.start()
        copies.append(copy)
        return copy

    handed = []

    def send_kv(owner, to, part=None):
        at = (owner,) if part is None else (owner, part)
        return send(kv_all.at[at], kv_all.at[at], to)

    def hand_kv(owner):
        handed.append(send_kv(owner, sib))

    def hand(slot):
        handed.append(send(cq_all.at[slot, 0], cq_all.at[slot, 1], sib))
        handed.append(send(tab_all.at[slot, 0], tab_all.at[slot, 1], sib))

    own = [pltpu.make_async_copy(tab_ref, tab_all.at[0, 0], loc.at[2])]
    own[0].start()
    tab_in = {s: send(tab_ref, tab_all.at[s, 0], square[s]) for s in (1, 2, 3)}
    handed.append(send(tab_ref, tab_all.at[0, 1], sib))
    yield

    own.append(pltpu.make_async_copy(kv_ref, kv_all.at[me], loc.at[0]))
    own[1].start()
    first_r = send(kv_ref, kv_all.at[me], right1)
    first_l = send(kv_ref, kv_all.at[me], left1)
    second = {0: (send(kv_ref, kv_all.at[me], right2), send(kv_ref, kv_all.at[me], left2))}
    handed.append(send(kv_ref, kv_all.at[me], sib))
    yield

    first_r.wait_recv()
    far_r = send_kv(left1, right1, 0)
    second[-1] = (send_kv(left1, right2), send_kv(left1, left2))
    hand_kv(left1)
    first_l.wait_recv()
    far_l = send_kv(right1, left1, 1)
    second[1] = (send_kv(right1, right2), send_kv(right1, left2))
    hand_kv(right1)

    yield

    own.append(pltpu.make_async_copy(cq_ref, cq_all.at[0, 0], loc.at[1]))
    own[2].start()
    cq_in = {s: send(cq_ref, cq_all.at[s, 0], square[s]) for s in (1, 2)}
    handed.append(send(cq_ref, cq_all.at[0, 1], sib))

    def pass_on(first):
        r, l = second[first]
        below, above = near(first, -1), near(first, 1)
        r.wait_recv()
        up = send_kv(below, right2, 0)
        hand_kv(below)
        l.wait_recv()
        down = send_kv(above, left2, 1)
        hand_kv(above)
        return up, down

    last = {0: pass_on(0)}
    far = near(2, 0)
    far_r.wait_recv()
    far_l.wait_recv()
    second[2] = (send_kv(far, right2), send_kv(far, left2))
    hand_kv(far)

    cq_in[1].wait_recv()
    tab_in[1].wait_recv()
    diag_a = send(cq_all.at[1, 0, 0], cq_all.at[3, 0, 0], square[2])
    hand(1)
    cq_in[2].wait_recv()
    tab_in[2].wait_recv()
    diag_b = send(cq_all.at[2, 0, 1], cq_all.at[3, 0, 1], square[1])
    hand(2)

    for first in (-1, 1, 2):
        last[first] = pass_on(first)
    diag_a.wait_recv()
    diag_b.wait_recv()
    tab_in[3].wait_recv()
    hand(3)
    for first in (0, -1, 1, 2):
        for copy in last[first]:
            copy.wait_recv()
        hand_kv(near(first, 2))
    for copy in handed:
        copy.wait_recv()
    for copy in copies:
        copy.wait_send()
    for copy in own:
        copy.wait()
    yield


N_COPIES = 4 + 3 + 2 + 3 + 2 + 4 * 2 + 2 * 3 + 15 + 2 + 6


def block_kernel(
    x1_ref, x2_ref, seg1_ref, pos1_ref, seg2_ref, pos2_ref, freq_ref, gq_ref, gkv_ref, wqd_ref, wkvd_ref, wqup_ref, wkvup_ref, wout_ref, y_ref,
    x_ref, kvd_buf, q_raw, cq_ref, kv_ref0, tab_ref0,
    cq_ref_all, kv_ref, tab_ref, wq_buf, wkv_buf, wo_buf, o_ref, o_in, y_own, y_far, y_in,
    kcat_ref, v_ref, qcat_ref, s_ref, p_ref, mask_ref,
    loc, g_send, g_recv, w_sem, wo_sem, o_send_sem, o_recv_sem, y_send_sem, y_recv_sem,
):
    where = place()
    me, core, sib, square, corner, near = where
    devs, _, rows, _ = kv_ref.shape
    keys = devs * rows
    q_lat = cq_ref_all.shape[-1]
    chip_rows = CORES * rows
    q_rows = CHIPS * chip_rows
    key_devs = devs // 8
    key_chunk = key_devs * rows
    soft_rows = SOFT_ROWS
    steps = o_ref.shape[1]
    heads = wqup_ref.shape[1] // QK_DIM
    my_heads = heads // MEMBERS
    n_blocks, _, blk = y_in.shape
    slots = wo_buf.shape[0]
    to_exp2 = QK_DIM ** -0.5 * 1.4426950408889634

    def first_head(d):
        return core * (heads // CORES) + corner[d] * my_heads

    def weight_copies(i):
        slot = i % 2
        h = first_head(0) + HEADS_PER_STEP * i
        wq, wkv = HEADS_PER_STEP * QK_DIM, HEADS_PER_STEP * KV_HEAD
        return (
            pltpu.make_async_copy(wqup_ref.at[:, pl.ds(pl.multiple_of(h * QK_DIM, LANES), wq)], wq_buf.at[slot], w_sem.at[slot, 0]),
            pltpu.make_async_copy(wkvup_ref.at[:, pl.ds(pl.multiple_of(h * KV_HEAD, LANES), wkv)], wkv_buf.at[slot], w_sem.at[slot, 1]),
        )

    def out_copies(b):
        slot = b % slots
        depth = my_heads * V_DIM
        return [
            pltpu.make_async_copy(
                wout_ref.at[pl.ds(pl.multiple_of(first_head(d) * V_DIM, depth), depth), pl.ds(pl.multiple_of(b * blk, LANES), blk)],
                wo_buf.at[slot, d],
                wo_sem.at[slot, d],
            )
            for d in range(CHIPS)
        ]

    depth = wqd_ref.shape[0]
    part = wo_buf.shape[2]
    cuts = [(d, d * part, min(part, depth - d * part)) for d in range((depth + part - 1) // part)]

    def down_copies(n):
        return [
            pltpu.make_async_copy(
                wqd_ref.at[at:at + size, n * blk:(n + 1) * blk], wo_buf.at[n, d, 0:size], wo_sem.at[n, d]
            )
            for d, at, size in cuts
        ]

    kv_down = pltpu.make_async_copy(wkvd_ref, kvd_buf, loc.at[3])
    kv_down.start()
    q_blocks = q_lat // blk
    for n in range(q_blocks):
        for copy in down_copies(n):
            copy.start()
    for copy in weight_copies(0):
        copy.start()


    def column(ref):
        square_at = lambda axis: lax.broadcasted_iota(jnp.int32, (rows, rows), axis)
        spread = jnp.broadcast_to(ref[...].astype(jnp.float32)[None, :], (rows, rows))
        return jnp.sum(jnp.where(square_at(0) == square_at(1), spread, 0.0), axis=1, keepdims=True)

    lane = lax.broadcasted_iota(jnp.int32, (rows, LANES), 1)
    tags = []
    for mb, (seg_in, pos_in) in enumerate(((seg1_ref, pos1_ref), (seg2_ref, pos2_ref))):
        seg, pos = column(seg_in), column(pos_in)
        angle = pos * freq_ref[...]
        sign = jnp.where(lane < ROPE_DIM + ROPE_DIM // 2, -1.0, 1.0)
        tab_ref0[mb] = jnp.where(lane < ROPE_DIM, jnp.cos(angle), sign * jnp.sin(angle))
        high = jnp.floor(pos * (1.0 / 32.0))
        tag = jnp.where(lane == 1, high, jnp.where(lane == 2, pos - 32.0 * high, 0.0))
        tags.append(jnp.where(lane == 0, seg, tag)[:, :LANES - ROPE_DIM])
    x_ref[:rows] = x1_ref[...]
    x_ref[rows:] = x2_ref[...]
    meet((sib, square[3], near(1, 0), near(-1, 0), near(0, 1), near(0, -1)))
    flow = gather(where, cq_ref, kv_ref0, tab_ref0, cq_ref_all, kv_ref, tab_ref, loc, g_send, g_recv)
    next(flow)

    def norm(z, gain):
        mean_sq = jnp.mean(z * z, axis=-1, keepdims=True)
        return (z * lax.rsqrt(mean_sq + NORM_EPS) * gain[...].astype(jnp.float32)[None, :]).astype(jnp.bfloat16)

    def turn(z, tab):
        turned = jnp.concatenate([z[:, ROPE_DIM // 2:], z[:, :ROPE_DIM // 2]], axis=1)
        return z * tab[:, :ROPE_DIM] + turned * tab[:, ROPE_DIM:]

    kv_down.wait()
    u = lax.dot_general(x_ref[...], kvd_buf[...], (((1,), (1,)), ((), ())), preferred_element_type=jnp.float32)
    latent = norm(u[:, :KV_LAT], gkv_ref)
    k_rope = turn(u[:, KV_LAT:], tab_ref0[...].reshape(MICRO * rows, LANES))
    packed = jnp.concatenate([latent, jnp.concatenate([k_rope, jnp.concatenate(tags, axis=0)], axis=1).astype(jnp.bfloat16)], axis=1)
    kv_ref0[...] = packed.reshape(kv_ref0.shape)
    next(flow)
    for n in range(q_blocks):
        for copy in down_copies(n):
            copy.wait()
        total = None
        for d, at, size in cuts:
            term = jnp.dot(x_ref[:, at:at + size], wo_buf[n, d, 0:size], preferred_element_type=jnp.float32)
            total = term if total is None else total + term
        q_raw[:, n * blk:(n + 1) * blk] = total
        for copy in out_copies(n):
            copy.start()
        if n == q_blocks - 3:
            next(flow)
    for n in range(q_blocks, slots):
        for copy in out_copies(n):
            copy.start()
    cq_ref[...] = norm(q_raw[...], gq_ref).reshape(cq_ref.shape)
    next(flow)

    lane = lax.broadcasted_iota(jnp.int32, (LANES, LANES), 1)
    weight = jnp.where(lane == ROPE_DIM, float(keys), jnp.where(lane == ROPE_DIM + 1, 32.0, jnp.where(lane == ROPE_DIM + 2, 1.0, 0.0)))
    weight_pos = jnp.where(lane == ROPE_DIM, 0.0, weight)
    nt = (((1,), (1,)), ((), ()))
    for mb in range(MICRO):
        tail = kv_ref[:, mb, :, KV_LAT:].reshape(keys, LANES)
        for par in range(HEADS_PER_STEP):
            kcat_ref[par, mb, :, NOPE_DIM:] = tail
        k_code = lax.dot_general(weight.astype(jnp.bfloat16), tail, nt, preferred_element_type=jnp.float32)
        for r in range(MEMBERS):
            owner = square[r // CORES] + (r % CORES) * (1 - 2 * core)
            mine = kv_ref[owner, mb, :, KV_LAT:]
            q_code = lax.dot_general(mine, weight.astype(jnp.bfloat16), nt, preferred_element_type=jnp.float32)
            q_pos = lax.dot_general(mine, weight_pos.astype(jnp.bfloat16), nt, preferred_element_type=jnp.float32)
            hi = q_code[:, :1]
            lo = (q_code - q_pos)[:, :1]
            row = k_code[:1, :]
            mask_ref[mb, r * rows:(r + 1) * rows, :] = jnp.where((row >= lo) & (row <= hi), 1.0, 0.0)

    def kv_part(slot, par, c):
        latent = kv_ref[c * key_devs:(c + 1) * key_devs, :, :, :KV_LAT].reshape(key_devs * MICRO * rows, KV_LAT)
        kv = jnp.dot(latent, wkv_buf[slot, :, par * KV_HEAD:(par + 1) * KV_HEAD], preferred_element_type=jnp.float32)
        kv = kv.astype(jnp.bfloat16).reshape(key_devs, MICRO, rows, KV_HEAD)
        for mb in range(MICRO):
            one = kv[:, mb].reshape(key_chunk, KV_HEAD)
            kcat_ref[par, mb, c * key_chunk:(c + 1) * key_chunk, :NOPE_DIM] = one[:, :NOPE_DIM]
            v_ref[par, mb, c * key_chunk:(c + 1) * key_chunk, :] = one[:, NOPE_DIM:]

    def q_part(slot, par, d):
        cq = cq_ref_all[d].reshape(CORES * MICRO * rows, q_lat)
        f = jnp.dot(cq, wq_buf[slot, :, par * QK_DIM:(par + 1) * QK_DIM], preferred_element_type=jnp.float32)
        tab = tab_ref[d].reshape(CORES * MICRO * rows, 2 * ROPE_DIM)
        z = f[:, NOPE_DIM:]
        turned = jnp.concatenate([z[:, ROPE_DIM // 2:], z[:, :ROPE_DIM // 2]], axis=1)
        rot = z * tab[:, :ROPE_DIM] + turned * tab[:, ROPE_DIM:]
        pad = jnp.zeros((rot.shape[0], LANES - ROPE_DIM), jnp.float32)
        q = jnp.concatenate([f[:, :NOPE_DIM], rot, pad], axis=1).astype(jnp.bfloat16)
        q = q.reshape(CORES, MICRO, rows, NOPE_DIM + LANES)
        for mb in range(MICRO):
            qcat_ref[par, mb, d * chip_rows:(d + 1) * chip_rows, :] = q[:, mb].reshape(chip_rows, NOPE_DIM + LANES)

    def score_part(par, mb, n):
        cols = slice(n * 256, (n + 1) * 256)
        s_ref[par, mb, :, cols] = lax.dot_general(
            qcat_ref[par, mb], kcat_ref[par, mb, cols, :], (((1,), (1,)), ((), ())), preferred_element_type=jnp.float32
        )

    def soft_part(par, mb, r):
        at = slice(r * soft_rows, (r + 1) * soft_rows)
        s = jnp.where(mask_ref[mb, at, :] > 0.5, s_ref[par, mb, at, :], -1e30)
        e = jnp.exp2((s - jnp.max(s, axis=1, keepdims=True)) * to_exp2)
        p_ref[mb, at, :] = (e * (1.0 / jnp.sum(e, axis=1, keepdims=True))).astype(jnp.bfloat16)

    def value_part(par, mb, step):
        o = jnp.dot(p_ref[mb], v_ref[par, mb], preferred_element_type=jnp.float32).astype(jnp.bfloat16)
        o = o.reshape(CHIPS, CORES, rows, V_DIM)
        for d in range(CHIPS):
            o_ref[d, step, :, mb, :, par * V_DIM:(par + 1) * V_DIM] = o[d]

    def first_stage(slot, par):
        parts = [functools.partial(kv_part, slot, par, c) for c in range(8)]
        parts += [functools.partial(q_part, slot, par, d) for d in range(CHIPS)]
        parts += [functools.partial(score_part, par, mb, n) for mb in range(MICRO) for n in range(keys // 256)]
        return parts

    def second_stage(par, step):
        parts = []
        for mb in range(MICRO):
            parts += [functools.partial(soft_part, par, mb, r) for r in range(q_rows // soft_rows)]
            parts.append(functools.partial(value_part, par, mb, step))
        return parts

    def o_copies(step):
        return [
            pltpu.make_async_remote_copy(
                src_ref=o_ref.at[d, step],
                dst_ref=o_in.at[d - 1, step],
                send_sem=o_send_sem.at[d - 1, step],
                recv_sem=o_recv_sem.at[d - 1, step],
                device_id={"sp": square[d]},
                device_id_type=MESH,
            )
            for d in range(1, CHIPS)
        ]

    def beside(a, b):
        order = [((k + 0.5) / len(a), 0, f) for k, f in enumerate(a)] + [((k + 0.6) / len(b), 1, f) for k, f in enumerate(b)]
        for _, _, f in sorted(order, key=lambda v: v[:2]):
            f()

    @pl.loop(0, steps)
    def _(i):
        slot = i % 2
        before = jnp.maximum(i - 1, 0)
        for copy in weight_copies(i):
            copy.wait()

        @pl.when(i + 1 < steps)
        def _():
            for copy in weight_copies(i + 1):
                copy.start()

        beside(first_stage(slot, 0), second_stage(1, before))

        @pl.when(i > 0)
        def _():
            for copy in o_copies(before):
                copy.start()

        beside(first_stage(slot, 1), second_stage(0, i))

    for f in second_stage(1, steps - 1):
        f()
    for copy in o_copies(steps - 1):
        copy.start()

    @pl.loop(0, steps)
    def _(i):
        for copy in o_copies(i):
            copy.wait()

    def y_copy(b):
        return pltpu.make_async_remote_copy(
            src_ref=y_far.at[b], dst_ref=y_in.at[b], send_sem=y_send_sem.at[b], recv_sem=y_recv_sem.at[b], device_id={"sp": sib}, device_id_type=MESH
        )

    def finish(b):
        y_copy(b).wait()
        y = (y_own[b] + y_in[b]).astype(jnp.bfloat16)
        at = pl.ds(pl.multiple_of(b * blk, LANES), blk)
        y_ref[:, at] = y

    @pl.loop(0, n_blocks)
    def _(b):
        slot = b % slots
        for copy in out_copies(b):
            copy.wait()
        total = None
        for d in range(CHIPS):
            src = o_ref.at[0] if d == 0 else o_in.at[d - 1]
            o = jnp.concatenate([src[s].reshape(CORES * MICRO * rows, HEADS_PER_STEP * V_DIM) for s in range(steps)], axis=1)
            term = jnp.dot(o, wo_buf[slot, d], preferred_element_type=jnp.float32)
            total = term if total is None else total + term
        y_own[b] = total[:MICRO * rows]
        y_far[b] = total[MICRO * rows:]
        y_copy(b).start()

        @pl.when(b + slots < n_blocks)
        def _():
            for copy in out_copies(b + slots):
                copy.start()

        @pl.when(b >= LAG)
        def _():
            finish(b - LAG)

    @pl.loop(n_blocks - LAG, n_blocks)
    def _(b):
        finish(b)


def latent_block(x_one, x_two, seg_one, pos_one, seg_two, pos_two, freq, gain_q, gain_kv, w_qdown, w_kvdown, w_qup, w_kvup, w_out, group):
    rows = x_one.shape[0]
    keys = group * rows
    q_rows = MEMBERS * rows
    hw = HEADS_PER_STEP
    cq = (MICRO, rows, w_qdown.shape[1])
    kv = (MICRO, rows, KV_PACK)
    table = (MICRO, rows, LANES)
    heads = w_out.shape[0] // V_DIM
    steps = heads // MEMBERS // hw
    cols = w_out.shape[1]
    n_blocks = cols // OUT_COLS
    out = jax.ShapeDtypeStruct((MICRO * rows, cols), jnp.bfloat16)
    dma = pltpu.SemaphoreType.DMA
    vmem, anywhere = pl.BlockSpec(memory_space=pltpu.VMEM), pl.BlockSpec(memory_space=pl.ANY)
    pair = (steps, CORES, MICRO, rows, hw * V_DIM)
    bf16, f32 = jnp.bfloat16, jnp.float32
    return pl.pallas_call(
        block_kernel,
        out_shape=out,
        in_specs=[vmem] * 9 + [anywhere] * 5,
        out_specs=vmem,
        scratch_shapes=[
            pltpu.VMEM((MICRO * rows, x_one.shape[1]), bf16),
            pltpu.VMEM(w_kvdown.shape, bf16),
            pltpu.VMEM((MICRO * rows, w_qdown.shape[1]), f32),
            pltpu.VMEM(cq, bf16),
            pltpu.VMEM(kv, bf16),
            pltpu.VMEM(table, f32),
            pltpu.VMEM((CHIPS, CORES) + cq, bf16),
            pltpu.VMEM((group,) + kv, bf16),
            pltpu.VMEM((CHIPS, CORES) + table, f32),
            pltpu.VMEM((2, w_qup.shape[0], hw * QK_DIM), bf16),
            pltpu.VMEM((2, w_kvup.shape[0], hw * KV_HEAD), bf16),
            pltpu.VMEM((OUT_SLOTS, CHIPS, heads // MEMBERS * V_DIM, OUT_COLS), bf16),
            pltpu.VMEM((CHIPS,) + pair, bf16),
            pltpu.VMEM((CHIPS - 1,) + pair, bf16),
            pltpu.VMEM((n_blocks, MICRO * rows, OUT_COLS), f32),
            pltpu.VMEM((n_blocks, MICRO * rows, OUT_COLS), f32),
            pltpu.VMEM((n_blocks, MICRO * rows, OUT_COLS), f32),
            pltpu.VMEM((hw, MICRO, keys, NOPE_DIM + LANES), bf16),
            pltpu.VMEM((hw, MICRO, keys, V_DIM), bf16),
            pltpu.VMEM((hw, MICRO, q_rows, NOPE_DIM + LANES), bf16),
            pltpu.VMEM((hw, MICRO, q_rows, keys), f32),
            pltpu.VMEM((MICRO, q_rows, keys), bf16),
            pltpu.VMEM((MICRO, q_rows, keys), f32),
            dma((4,)),
            dma((N_COPIES,)),
            dma((N_COPIES,)),
            dma((2, 2)),
            dma((OUT_SLOTS, CHIPS)),
            dma((CHIPS - 1, steps)),
            dma((CHIPS - 1, steps)),
            dma((n_blocks,)),
            dma((n_blocks,)),
        ],
        compiler_params=pltpu.CompilerParams(collective_id=0, has_side_effects=True, vmem_limit_bytes=VMEM_LIMIT),
        name="latent_block",
    )(x_one, x_two, seg_one, pos_one, seg_two, pos_two, freq, gain_q, gain_kv, w_qdown, w_kvdown, w_qup, w_kvup, w_out)


def solution(mesh):
    tok_spec = P(("dp", "sp"), None)
    idx_spec = P(("dp", "sp"))
    group = mesh.shape["sp"]

    def local_body(x_one, seg_one, pos_one, x_two, seg_two, pos_two, w_qdown, gain_q, w_qup, w_kvdown, gain_kv, w_kvup, w_out):
        rows = x_one.shape[0]
        half = ROPE_DIM // 2
        inv_freq = np.float32(ROPE_BASE) ** (-np.arange(half, dtype=np.float32) / half)
        freq = np.tile(inv_freq, LANES // half)[None, :]
        y = latent_block(
            x_one, x_two, seg_one, pos_one, seg_two, pos_two, freq, gain_q, gain_kv, w_qdown, w_kvdown.T, w_qup, w_kvup, w_out, group
        )
        return y[:rows], y[rows:]

    rep = P()
    return jax.shard_map(
        local_body,
        mesh=mesh,
        in_specs=(tok_spec, idx_spec, idx_spec, tok_spec, idx_spec, idx_spec, rep, rep, rep, rep, rep, rep, rep),
        out_specs=(tok_spec, tok_spec),
        check_vma=False,
    )
```
